32 devices in a mesh: sweep: 2 (over y), seq: 8 (over z, x), head: 2 (over core).
Axes of the slice: x: 2, y: 2, z: 4, core: 2. Of those that a mesh axis runs over, the one named last changes fastest.
Arguments:
- queries: bfloat16 [2048, 1024], P(('sweep', 'seq'), 'head'), parts along dimension 0, may hold values from -6 to 6
- key_matrix: bfloat16 [2048, 256], P(('sweep', 'seq'), 'head'), parts along dimension 0, may hold values from -6 to 6
- value_matrix: bfloat16 [2048, 256], P(('sweep', 'seq'), 'head'), parts along dimension 0, may hold values from -6 to 6
- segment_ids: int32 [2048], P(('sweep', 'seq')), parts along dimension 0, may hold values from 0 to 16, as said below
Outputs:
- attended: bfloat16 [2048, 1024], P(('sweep', 'seq'), 'head'), parts along dimension 0
The draws below stay inside these ranges and needn't reach their ends.
There are 2 independent parts, one for each index of `sweep`. The reference program is written for one: setup_inputs(seed, part) draws one part's arguments, and reference() takes and returns one part's arrays. A program takes and returns all parts, laid end to end along the dimension named above; each array names one. Nothing has to cross between parts.
Inputs may be any that keep to these rules, and one draw needn't show every extreme that they name: `segment_ids`: never falling. Segment 0 is a prompt at the start of 128 to 256 tokens; each id of 1 to 16 is one response of one or more tokens.
All inputs are finite; a program needn't handle non-finite values.
Results may differ from the reference program's by a relative error of at most 0.005.
Values may be sent and summed in bfloat16 or wider, within the bound.
A program may use at most 64 MiB of HBM per device.

```python
import math
import jax
import jax.numpy as jnp
from jax import lax

QUERY_HEAD_COUNT = 16
KEY_VALUE_HEADS = 4
HEAD_WIDTH = 64
RESP = 16
TOKENS_PER_SHARD = 128
ROLLOUT_TOKENS = 1024
N_SEQ = 8


def draw_queries(key, part):
    base_offset = jnp.clip(jax.random.normal(jax.random.fold_in(key, 1), (ROLLOUT_TOKENS, QUERY_HEAD_COUNT * HEAD_WIDTH), jnp.float32), -6.0, 6.0)
    return base_offset.astype(jnp.bfloat16)


def draw_key_matrix(key, part):
    base_offset = jnp.clip(jax.random.normal(jax.random.fold_in(key, 2), (ROLLOUT_TOKENS, KEY_VALUE_HEADS * HEAD_WIDTH), jnp.float32), -6.0, 6.0)
    return base_offset.astype(jnp.bfloat16)


def draw_segment_ids(key, part):
    position = jnp.arange(ROLLOUT_TOKENS, dtype=jnp.int32)
    prompt = jax.random.randint(jax.random.fold_in(key, 21), (), ROLLOUT_TOKENS // 8, ROLLOUT_TOKENS // 4 + 1)
    later = jax.random.permutation(jax.random.fold_in(key, 22), jnp.arange(ROLLOUT_TOKENS // 4 + 1, ROLLOUT_TOKENS, dtype=jnp.int32))
    later = later[:RESP - 1]
    labels = (position >= prompt).astype(jnp.int32)
    labels = labels + jnp.sum((position[:, None] >= later[None, :]).astype(jnp.int32), axis=1)
    return labels.astype(jnp.int32)


def level_of(key, shape, cuts, low, high):
    gain = 1.0
    for axis_at, shards_of in cuts:
        steps = jax.random.uniform(jax.random.fold_in(jax.random.fold_in(key, 6), axis_at), (shards_of,), jnp.float32, low / len(cuts), high / len(cuts))
        gain = gain * jnp.repeat(jnp.exp(steps), shape[axis_at] // shards_of).reshape((-1,) + (1,) * (len(shape) - 1 - axis_at))
    return gain


def scatter_about(stream_key, extent, spread, most, pieces=(), held_as=jnp.bfloat16):
    gain = level_of(stream_key, extent, pieces, -0.22, 0.18) if pieces else 1.0
    values = jax.random.normal(stream_key, extent, jnp.float32) * spread * gain
    return jnp.minimum(jnp.maximum(values, -most), most).astype(held_as)


def setup_inputs(seed: int = 0, part: int = 0) -> dict:
    arg_keys = jax.random.split(jax.random.key(seed), 5)
    part_splits = jax.random.split(jax.random.fold_in(arg_keys[4], part), 5)
    return {
        "queries": draw_queries(jax.random.fold_in(jax.random.fold_in(arg_keys[4], part), 71), part),
        "key_matrix": draw_key_matrix(jax.random.fold_in(jax.random.fold_in(arg_keys[4], part), 71), part),
        "value_matrix": scatter_about(part_splits[2], (ROLLOUT_TOKENS, KEY_VALUE_HEADS * HEAD_WIDTH), 1.0, 6.0, ((0, 8), (1, 2))),
        "segment_ids": draw_segment_ids(jax.random.fold_in(jax.random.fold_in(arg_keys[4], part), 71), part),
    }


NEG_FILL = -1e+30

def reference(queries, key_matrix, value_matrix, segment_ids):
    repeat_factor = QUERY_HEAD_COUNT // KEY_VALUE_HEADS
    gathered_keys = key_matrix.reshape(ROLLOUT_TOKENS, KEY_VALUE_HEADS, HEAD_WIDTH).astype(jnp.float32)
    gathered_values = value_matrix.reshape(ROLLOUT_TOKENS, KEY_VALUE_HEADS, HEAD_WIDTH).astype(jnp.float32)
    key_pos = jnp.arange(ROLLOUT_TOKENS, dtype=jnp.int32)
    score_scale = 1.0 / math.sqrt(HEAD_WIDTH)

    def one_block(index):
        first = (index * TOKENS_PER_SHARD).astype(jnp.int32)
        query_block = lax.dynamic_slice_in_dim(queries, first, TOKENS_PER_SHARD, 0)
        query_block = query_block.reshape(TOKENS_PER_SHARD, KEY_VALUE_HEADS, repeat_factor, HEAD_WIDTH).astype(jnp.float32)
        query_seg = lax.dynamic_slice_in_dim(segment_ids, first, TOKENS_PER_SHARD, 0)
        query_pos = first + jnp.arange(TOKENS_PER_SHARD, dtype=jnp.int32)
        visible = (key_pos[None, :] <= query_pos[:, None]) & ((segment_ids[None, :] == query_seg[:, None]) | (segment_ids[None, :] == 0))
        logit_scores = jnp.einsum('opez,hpz->peoh', query_block, gathered_keys) * score_scale
        logit_scores = jnp.where(visible, logit_scores, NEG_FILL)
        top = lax.optimization_barrier(jnp.max(logit_scores, axis=-1, keepdims=True))
        weights = jnp.where(visible, jnp.exp(logit_scores - top), 0.0)
        weight_total = lax.optimization_barrier(jnp.sum(weights, axis=-1))
        rounded_scores = lax.optimization_barrier(weights.astype(jnp.bfloat16)).astype(jnp.float32)
        mixed_output = jnp.einsum('omhy,yoc->omhc', rounded_scores, gathered_values) / weight_total[..., None]
        result = jnp.transpose(mixed_output, (2, 0, 1, 3)).reshape(TOKENS_PER_SHARD, QUERY_HEAD_COUNT * HEAD_WIDTH)
        return result.astype(jnp.bfloat16)
    blocks = lax.map(one_block, jnp.arange(N_SEQ, dtype=jnp.int32))
    return blocks.reshape(ROLLOUT_TOKENS, QUERY_HEAD_COUNT * HEAD_WIDTH)
```

```python
import functools
import math

import jax
import jax.numpy as jnp
from jax import lax
from jax.experimental import pallas as pl
from jax.experimental.pallas import tpu as pltpu
from jax.sharding import PartitionSpec as P

HEAD_WIDTH = 64
NEG_FILL = -1e30
MESH = pl.DeviceIdType.MESH


def kernel(n, inner, q_hbm, k_hbm, v_hbm, s_hbm, o_ref, qv, kbuf, vbuf, sbuf, qm, run_max, acc,
           in_sem, col_sem, row_sem, recv_sem):
    rows = k_hbm.shape[0]
    width = k_hbm.shape[1]
    half = HEAD_WIDTH
    groups = width // half
    tiles = q_hbm.shape[1] // width
    per_group = tiles // groups
    outer = n // inner
    me = lax.axis_index("seq")
    z = me // inner
    x = me % inner
    partner = z * inner + (inner - 1 - x)
    bufs = (sbuf, kbuf, vbuf)

    loads = [
        pltpu.make_async_copy(src, dst, in_sem.at[i])
        for i, (src, dst) in enumerate(
            ((s_hbm, sbuf.at[me]), (k_hbm, kbuf.at[me]), (v_hbm, vbuf.at[me]), (q_hbm, qv))
        )
    ]
    for load in loads:
        load.start()

    barrier = pltpu.get_barrier_semaphore()

    def greet(i, c):
        other = (z + 1 + i) % outer
        pl.semaphore_signal(barrier, inc=1, device_id={"seq": other * inner + x}, device_id_type=MESH)
        return c

    if inner == 2:
        pl.semaphore_signal(barrier, inc=1, device_id={"seq": partner}, device_id_type=MESH)
    lax.fori_loop(0, outer - 1, greet, 0)
    pl.semaphore_wait(barrier, outer - 1 + inner - 1)

    def along_column(kind, target):
        return pltpu.make_async_remote_copy(
            src_ref=bufs[kind].at[me], dst_ref=bufs[kind].at[me],
            send_sem=col_sem.at[kind, target], recv_sem=recv_sem.at[kind, me],
            device_id={"seq": target * inner + x}, device_id_type=MESH)

    def across(kind, row):
        block = row * inner + x
        return pltpu.make_async_remote_copy(
            src_ref=bufs[kind].at[block], dst_ref=bufs[kind].at[block],
            send_sem=row_sem.at[kind, row], recv_sem=recv_sem.at[kind, block],
            device_id={"seq": partner}, device_id_type=MESH)

    def arrival(kind, block):
        return pltpu.make_async_remote_copy(
            src_ref=bufs[kind].at[block], dst_ref=bufs[kind].at[block],
            send_sem=col_sem.at[kind, z], recv_sem=recv_sem.at[kind, block],
            device_id={"seq": partner}, device_id_type=MESH)

    for load in loads[:3]:
        load.wait()
    if inner == 2:
        @pl.when(x == 0)
        def _():
            for kind in range(3):
                across(kind, z).start()

    def send_column(i, c):
        for kind in range(3):
            along_column(kind, outer - 1 - i).start()
        return c

    lax.fori_loop(0, outer - 1 - z, send_column, 0)
    loads[3].wait()

    scale = 1.0 / math.sqrt(half)
    zeros = jnp.zeros((rows, half), jnp.bfloat16)
    for g in range(groups):
        for i in range(per_group):
            at = (g * per_group + i) * width
            lo = (qv[:, at:at + half] * scale).astype(jnp.bfloat16)
            hi = (qv[:, at + half:at + width] * scale).astype(jnp.bfloat16)
            qm[g, i] = jnp.concatenate([lo, zeros], axis=1)
            qm[g, per_group + i] = jnp.concatenate([zeros, hi], axis=1)

    seg_q = jnp.transpose(jnp.broadcast_to(sbuf[me], (rows, rows)))

    def attend(kk, vv, vis, first):
        count = kk.shape[0]
        bias = jnp.where(vis, 0.0, NEG_FILL).astype(jnp.float32)
        ones = jnp.ones((count, half), jnp.bfloat16)
        for g in range(groups):
            kg = kk[:, g * half:(g + 1) * half]
            vg = vv[:, g * half:(g + 1) * half]
            kd = jnp.concatenate([kg, kg], axis=1)
            heads = 2 * per_group
            s = lax.dot_general(
                qm[g].reshape(heads * rows, width), kd, (((1,), (1,)), ((), ())),
                preferred_element_type=jnp.float32)
            s = s.reshape(heads, rows, count) + bias[None]
            top = jnp.max(s, axis=-1, keepdims=True)
            if first:
                new = jnp.broadcast_to(top, (heads, rows, rows))
            else:
                old = run_max[g]
                new = jnp.maximum(old, top)
            run_max[g] = new
            p = jnp.exp(s - jnp.concatenate([new] * (count // rows), axis=-1)).astype(jnp.bfloat16)
            sides = (jnp.concatenate([vg, ones], axis=1), jnp.concatenate([ones, vg], axis=1))
            for side in range(2):
                part = slice(side * per_group, (side + 1) * per_group)
                mixed = jnp.dot(
                    p[part].reshape(per_group * rows, count), sides[side],
                    preferred_element_type=jnp.float32).reshape(per_group, rows, width)
                if first:
                    acc[g, part] = mixed
                else:
                    acc[g, part] = acc[g, part] * jnp.exp(old[part] - new[part]) + mixed

    row_at = lax.broadcasted_iota(jnp.int32, (rows, rows), 0)
    col_at = lax.broadcasted_iota(jnp.int32, (rows, rows), 1)
    seg_k = jnp.broadcast_to(sbuf[me], (rows, rows))
    attend(kbuf[me], vbuf[me], (col_at <= row_at) & ((seg_k == seg_q) | (seg_k == 0)), True)

    def seen(seg):
        seg = jnp.broadcast_to(seg, (rows, rows))
        return (seg == seg_q) | (seg == 0)

    def take(row):
        for kind in range(3):
            arrival(kind, row * inner + x).wait_recv()
            if inner == 2:
                across(kind, row).start()

    @pl.when(z > 0)
    def _():
        take(z - 1)

    if inner == 2:
        @pl.when(x == 1)
        def _():
            for kind in range(3):
                arrival(kind, partner).wait_recv()
            attend(kbuf[partner], vbuf[partner], seen(sbuf[partner]), False)

    def step(i, c):
        row = z - 1 - i

        @pl.when(row > 0)
        def _():
            take(row - 1)

        if inner == 2:
            for kind in range(3):
                arrival(kind, row * inner + 1 - x).wait_recv()
        first = row * inner
        kk = kbuf[pl.ds(first, inner)].reshape(inner * rows, width)
        vv = vbuf[pl.ds(first, inner)].reshape(inner * rows, width)
        vis = jnp.concatenate(
            [jnp.where(seen(sbuf[first + i]), 1, 0) for i in range(inner)], axis=1) == 1
        attend(kk, vv, vis, False)
        return c

    lax.fori_loop(0, z, step, 0)

    left = lax.broadcasted_iota(jnp.int32, (rows, width), 1) < half
    for g in range(groups):
        for i in range(per_group):
            a = acc[g, i]
            b = acc[g, per_group + i]
            total = pltpu.roll(jnp.where(left, b, a), half, 1)
            at = (g * per_group + i) * width
            o_ref[:, at:at + width] = (jnp.where(left, a, b) / total).astype(o_ref.dtype)

    if inner == 2:
        @pl.when(x == 0)
        def _():
            for kind in range(3):
                across(kind, z).wait_send()

        def drain_row(row, c):
            for kind in range(3):
                across(kind, row).wait_send()
            return c

        lax.fori_loop(0, z, drain_row, 0)

    def drain_column(i, c):
        for kind in range(3):
            along_column(kind, outer - 1 - i).wait_send()
        return c

    lax.fori_loop(0, outer - 1 - z, drain_column, 0)


def per_device(n, queries, key_matrix, value_matrix, segment_ids):
    rows, width = key_matrix.shape
    inner = 2 if n % 2 == 0 else 1
    groups = width // HEAD_WIDTH
    heads = queries.shape[1] // HEAD_WIDTH // groups
    return pl.pallas_call(
        functools.partial(kernel, n, inner),
        out_shape=jax.ShapeDtypeStruct(queries.shape, jnp.bfloat16),
        in_specs=[pl.BlockSpec(memory_space=pl.ANY)] * 4,
        out_specs=pl.BlockSpec(memory_space=pltpu.VMEM),
        scratch_shapes=[
            pltpu.VMEM(queries.shape, jnp.bfloat16),
            pltpu.VMEM((n, rows, width), jnp.bfloat16),
            pltpu.VMEM((n, rows, width), jnp.bfloat16),
            pltpu.VMEM((n, 1, rows), jnp.int32),
            pltpu.VMEM((groups, heads, rows, width), jnp.bfloat16),
            pltpu.VMEM((groups, heads, rows, rows), jnp.float32),
            pltpu.VMEM((groups, heads, rows, width), jnp.float32),
            pltpu.SemaphoreType.DMA((4,)),
            pltpu.SemaphoreType.DMA((3, n // inner)),
            pltpu.SemaphoreType.DMA((3, n // inner)),
            pltpu.SemaphoreType.DMA((3, n)),
        ],
        compiler_params=pltpu.CompilerParams(collective_id=0, has_side_effects=True),
    )(queries, key_matrix, value_matrix, segment_ids.reshape(1, rows))


def solution(mesh):
    blocks = P(("sweep", "seq"), "head")
    return jax.shard_map(
        functools.partial(per_device, mesh.shape["seq"]),
        mesh=mesh,
        in_specs=(blocks, blocks, blocks, P(("sweep", "seq"))),
        out_specs=blocks,
        check_vma=False,
    )
```

```python
import functools
import math

import jax
import jax.numpy as jnp
from jax import lax
from jax.experimental import pallas as pl
from jax.experimental.pallas import tpu as pltpu
from jax.sharding import PartitionSpec as P

HEAD_WIDTH = 64
NEG_FILL = -1e30
MESH = pl.DeviceIdType.MESH


def kernel(n, inner, q_hbm, k_hbm, v_hbm, s_hbm, o_ref, qv, kbuf, vbuf, sbuf, qm, run_max, acc,
           in_sem, col_sem, row_sem, recv_sem):
    rows = k_hbm.shape[0]
    width = k_hbm.shape[1]
    half = HEAD_WIDTH
    groups = width // half
    tiles = q_hbm.shape[1] // width
    per_group = tiles // groups
    outer = n // inner
    me = lax.axis_index("seq")
    z = me // inner
    x = me % inner
    partner = z * inner + (inner - 1 - x)
    bufs = (sbuf, kbuf, vbuf)

    loads = [
        pltpu.make_async_copy(src, dst, in_sem.at[i])
        for i, (src, dst) in enumerate(
            ((s_hbm, sbuf.at[me]), (k_hbm, kbuf.at[me]), (v_hbm, vbuf.at[me]), (q_hbm, qv))
        )
    ]
    for load in loads:
        load.start()

    barrier = pltpu.get_barrier_semaphore()

    if inner == 2:
        pl.semaphore_signal(barrier, inc=1, device_id={"seq": partner}, device_id_type=MESH)

    @pl.when(z > 0)
    def _():
        pl.semaphore_signal(barrier, inc=1, device_id={"seq": me - inner}, device_id_type=MESH)

    pl.semaphore_wait(barrier, inner - 1 + jnp.where(z < outer - 1, 1, 0))

    def onward(kind, row):
        block = row * inner + x
        return pltpu.make_async_remote_copy(
            src_ref=bufs[kind].at[block], dst_ref=bufs[kind].at[block],
            send_sem=col_sem.at[kind, row], recv_sem=recv_sem.at[kind, block],
            device_id={"seq": me + inner}, device_id_type=MESH)

    def across(kind, row):
        block = row * inner + x
        return pltpu.make_async_remote_copy(
            src_ref=bufs[kind].at[block], dst_ref=bufs[kind].at[block],
            send_sem=row_sem.at[kind, row], recv_sem=recv_sem.at[kind, block],
            device_id={"seq": partner}, device_id_type=MESH)

    def arrival(kind, block):
        return pltpu.make_async_remote_copy(
            src_ref=bufs[kind].at[block], dst_ref=bufs[kind].at[block],
            send_sem=in_sem.at[0], recv_sem=recv_sem.at[kind, block],
            device_id={"seq": partner}, device_id_type=MESH)

    for kind in range(3):
        loads[kind].wait()

        @pl.when(z < outer - 1)
        def _():
            onward(kind, z).start()

        if inner == 2:
            @pl.when(x == 0)
            def _():
                across(kind, z).start()

    loads[3].wait()

    scale = 1.0 / math.sqrt(half)
    zeros = jnp.zeros((rows, half), jnp.bfloat16)
    for g in range(groups):
        for i in range(per_group):
            at = (g * per_group + i) * width
            lo = (qv[:, at:at + half] * scale).astype(jnp.bfloat16)
            hi = (qv[:, at + half:at + width] * scale).astype(jnp.bfloat16)
            qm[g, i] = jnp.concatenate([lo, zeros], axis=1)
            qm[g, per_group + i] = jnp.concatenate([zeros, hi], axis=1)

    seg_q = jnp.transpose(jnp.broadcast_to(sbuf[me], (rows, rows)))

    def attend(kk, vv, vis, first):
        count = kk.shape[0]
        bias = jnp.where(vis, 0.0, NEG_FILL).astype(jnp.float32)
        ones = jnp.ones((count, half), jnp.bfloat16)
        for g in range(groups):
            kg = kk[:, g * half:(g + 1) * half]
            vg = vv[:, g * half:(g + 1) * half]
            kd = jnp.concatenate([kg, kg], axis=1)
            heads = 2 * per_group
            s = lax.dot_general(
                qm[g].reshape(heads * rows, width), kd, (((1,), (1,)), ((), ())),
                preferred_element_type=jnp.float32)
            s = s.reshape(heads, rows, count) + bias[None]
            top = jnp.max(s, axis=-1, keepdims=True)
            if first:
                new = jnp.broadcast_to(top, (heads, rows, rows))
            else:
                old = run_max[g]
                new = jnp.maximum(old, top)
            run_max[g] = new
            p = jnp.exp(s - jnp.concatenate([new] * (count // rows), axis=-1)).astype(jnp.bfloat16)
            sides = (jnp.concatenate([vg, ones], axis=1), jnp.concatenate([ones, vg], axis=1))
            for side in range(2):
                part = slice(side * per_group, (side + 1) * per_group)
                mixed = jnp.dot(
                    p[part].reshape(per_group * rows, count), sides[side],
                    preferred_element_type=jnp.float32).reshape(per_group, rows, width)
                if first:
                    acc[g, part] = mixed
                else:
                    acc[g, part] = acc[g, part] * jnp.exp(old[part] - new[part]) + mixed

    row_at = lax.broadcasted_iota(jnp.int32, (rows, rows), 0)
    col_at = lax.broadcasted_iota(jnp.int32, (rows, rows), 1)
    seg_k = jnp.broadcast_to(sbuf[me], (rows, rows))
    attend(kbuf[me], vbuf[me], (col_at <= row_at) & ((seg_k == seg_q) | (seg_k == 0)), True)

    def seen(seg):
        seg = jnp.broadcast_to(seg, (rows, rows))
        return (seg == seg_q) | (seg == 0)

    def take(i, c):
        row = z - 1 - i
        for kind in range(3):
            arrival(kind, row * inner + x).wait_recv()

            @pl.when(z < outer - 1)
            def _():
                onward(kind, row).start()

            if inner == 2:
                across(kind, row).start()
        return c

    @pl.when(z > 0)
    def _():
        take(0, 0)

    if inner == 2:
        @pl.when(x == 1)
        def _():
            for kind in range(3):
                arrival(kind, partner).wait_recv()
            attend(kbuf[partner], vbuf[partner], seen(sbuf[partner]), False)

    lax.fori_loop(1, z, take, 0)

    def step(i, c):
        row = z - 1 - i
        if inner == 2:
            for kind in range(3):
                arrival(kind, row * inner + 1 - x).wait_recv()
        first = row * inner
        kk = kbuf[pl.ds(first, inner)].reshape(inner * rows, width)
        vv = vbuf[pl.ds(first, inner)].reshape(inner * rows, width)
        vis = jnp.concatenate(
            [jnp.where(seen(sbuf[first + i]), 1, 0) for i in range(inner)], axis=1) == 1
        attend(kk, vv, vis, False)
        return c

    lax.fori_loop(0, z, step, 0)

    left = lax.broadcasted_iota(jnp.int32, (rows, width), 1) < half
    for g in range(groups):
        for i in range(per_group):
            a = acc[g, i]
            b = acc[g, per_group + i]
            total = pltpu.roll(jnp.where(left, b, a), half, 1)
            at = (g * per_group + i) * width
            o_ref[:, at:at + width] = (jnp.where(left, a, b) / total).astype(o_ref.dtype)

    if inner == 2:
        @pl.when(x == 0)
        def _():
            for kind in range(3):
                across(kind, z).wait_send()

        def drain_row(row, c):
            for kind in range(3):
                across(kind, row).wait_send()
            return c

        lax.fori_loop(0, z, drain_row, 0)

    @pl.when(z < outer - 1)
    def _():
        def drain_column(row, c):
            for kind in range(3):
                onward(kind, row).wait_send()
            return c

        lax.fori_loop(0, z + 1, drain_column, 0)


def per_device(n, queries, key_matrix, value_matrix, segment_ids):
    rows, width = key_matrix.shape
    inner = 2 if n % 2 == 0 else 1
    groups = width // HEAD_WIDTH
    heads = queries.shape[1] // HEAD_WIDTH // groups
    return pl.pallas_call(
        functools.partial(kernel, n, inner),
        out_shape=pltpu.VMEM(queries.shape, jnp.bfloat16),
        in_specs=[pl.BlockSpec(memory_space=pl.ANY)] * 4,
        out_specs=pl.BlockSpec(memory_space=pltpu.VMEM),
        scratch_shapes=[
            pltpu.VMEM(queries.shape, jnp.bfloat16),
            pltpu.VMEM((n, rows, width), jnp.bfloat16),
            pltpu.VMEM((n, rows, width), jnp.bfloat16),
            pltpu.VMEM((n, 1, rows), jnp.int32),
            pltpu.VMEM((groups, heads, rows, width), jnp.bfloat16),
            pltpu.VMEM((groups, heads, rows, rows), jnp.float32),
            pltpu.VMEM((groups, heads, rows, width), jnp.float32),
            pltpu.SemaphoreType.DMA((4,)),
            pltpu.SemaphoreType.DMA((3, n // inner)),
            pltpu.SemaphoreType.DMA((3, n // inner)),
            pltpu.SemaphoreType.DMA((3, n)),
        ],
        compiler_params=pltpu.CompilerParams(collective_id=0, has_side_effects=True),
    )(queries, key_matrix, value_matrix, segment_ids.reshape(1, rows))


def solution(mesh):
    blocks = P(("sweep", "seq"), "head")
    return jax.shard_map(
        functools.partial(per_device, mesh.shape["seq"]),
        mesh=mesh,
        in_specs=(blocks, blocks, blocks, P(("sweep", "seq"))),
        out_specs=blocks,
        check_vma=False,
    )
```

```python
import functools
import math

import jax
import jax.numpy as jnp
from jax import lax
from jax.experimental import pallas as pl
from jax.experimental.pallas import tpu as pltpu
from jax.sharding import PartitionSpec as P

HEAD_WIDTH = 64
NEG_FILL = -1e30
MESH = pl.DeviceIdType.MESH
PIECES = 2


def kernel(n, inner, q_hbm, k_hbm, v_hbm, s_hbm, o_ref, qv, kbuf, vbuf, sbuf, qm, run_max, acc,
           in_sem, col_sem, row_sem, recv_sem):
    rows = k_hbm.shape[0]
    width = k_hbm.shape[1]
    half = HEAD_WIDTH
    groups = width // half
    tiles = q_hbm.shape[1] // width
    per_group = tiles // groups
    outer = n // inner
    me = lax.axis_index("seq")
    z = me // inner
    x = me % inner
    partner = z * inner + (inner - 1 - x)
    kinds = 1 + 2 * PIECES
    size = rows // PIECES

    def piece(kind, block):
        if kind == 0:
            return sbuf.at[block]
        buf = kbuf if kind <= PIECES else vbuf
        return buf.at[block, pl.ds((kind - 1) % PIECES * size, size)]


    loads = [
        pltpu.make_async_copy(src, dst, in_sem.at[i])
        for i, (src, dst) in enumerate(
            ((s_hbm, sbuf.at[me]), (k_hbm, kbuf.at[me]), (v_hbm, vbuf.at[me]), (q_hbm, qv))
        )
    ]
    for load in loads:
        load.start()

    barrier = pltpu.get_barrier_semaphore()

    if inner == 2:
        pl.semaphore_signal(barrier, inc=1, device_id={"seq": partner}, device_id_type=MESH)

    @pl.when(z > 0)
    def _():
        pl.semaphore_signal(barrier, inc=1, device_id={"seq": me - inner}, device_id_type=MESH)

    pl.semaphore_wait(barrier, inner - 1 + jnp.where(z < outer - 1, 1, 0))

    def onward(kind, row):
        block = row * inner + x
        return pltpu.make_async_remote_copy(
            src_ref=piece(kind, block), dst_ref=piece(kind, block),
            send_sem=col_sem.at[kind, row], recv_sem=recv_sem.at[kind, block],
            device_id={"seq": me + inner}, device_id_type=MESH)

    def across(kind, row):
        block = row * inner + x
        return pltpu.make_async_remote_copy(
            src_ref=piece(kind, block), dst_ref=piece(kind, block),
            send_sem=row_sem.at[kind, row], recv_sem=recv_sem.at[kind, block],
            device_id={"seq": partner}, device_id_type=MESH)

    def arrival(kind, block):
        return pltpu.make_async_remote_copy(
            src_ref=piece(kind, block), dst_ref=piece(kind, block),
            send_sem=in_sem.at[0], recv_sem=recv_sem.at[kind, block],
            device_id={"seq": partner}, device_id_type=MESH)

    for kind in range(kinds):
        if kind in (0, 1, 1 + PIECES):
            loads[(0, 1, 1 + PIECES).index(kind)].wait()

        @pl.when(z < outer - 1)
        def _():
            onward(kind, z).start()

        if inner == 2:
            @pl.when(x == 0)
            def _():
                across(kind, z).start()

    loads[3].wait()

    scale = 1.0 / math.sqrt(half)
    zeros = jnp.zeros((rows, half), jnp.bfloat16)
    for g in range(groups):
        for i in range(per_group):
            at = (g * per_group + i) * width
            lo = (qv[:, at:at + half] * scale).astype(jnp.bfloat16)
            hi = (qv[:, at + half:at + width] * scale).astype(jnp.bfloat16)
            qm[g, i] = jnp.concatenate([lo, zeros], axis=1)
            qm[g, per_group + i] = jnp.concatenate([zeros, hi], axis=1)

    seg_q = jnp.transpose(jnp.broadcast_to(sbuf[me], (rows, rows)))

    def attend(kk, vv, vis, first):
        count = kk.shape[0]
        bias = jnp.where(vis, 0.0, NEG_FILL).astype(jnp.float32)
        ones = jnp.ones((count, half), jnp.bfloat16)
        for g in range(groups):
            kg = kk[:, g * half:(g + 1) * half]
            vg = vv[:, g * half:(g + 1) * half]
            kd = jnp.concatenate([kg, kg], axis=1)
            heads = 2 * per_group
            s = lax.dot_general(
                qm[g].reshape(heads * rows, width), kd, (((1,), (1,)), ((), ())),
                preferred_element_type=jnp.float32)
            s = s.reshape(heads, rows, count) + bias[None]
            top = jnp.max(s, axis=-1, keepdims=True)
            if first:
                new = jnp.broadcast_to(top, (heads, rows, rows))
            else:
                old = run_max[g]
                new = jnp.maximum(old, top)
            run_max[g] = new
            p = jnp.exp(s - jnp.concatenate([new] * (count // rows), axis=-1)).astype(jnp.bfloat16)
            sides = (jnp.concatenate([vg, ones], axis=1), jnp.concatenate([ones, vg], axis=1))
            for side in range(2):
                part = slice(side * per_group, (side + 1) * per_group)
                mixed = jnp.dot(
                    p[part].reshape(per_group * rows, count), sides[side],
                    preferred_element_type=jnp.float32).reshape(per_group, rows, width)
                if first:
                    acc[g, part] = mixed
                else:
                    acc[g, part] = acc[g, part] * jnp.exp(old[part] - new[part]) + mixed

    row_at = lax.broadcasted_iota(jnp.int32, (rows, rows), 0)
    col_at = lax.broadcasted_iota(jnp.int32, (rows, rows), 1)
    seg_k = jnp.broadcast_to(sbuf[me], (rows, rows))
    attend(kbuf[me], vbuf[me], (col_at <= row_at) & ((seg_k == seg_q) | (seg_k == 0)), True)

    def seen(seg):
        seg = jnp.broadcast_to(seg, (rows, rows))
        return (seg == seg_q) | (seg == 0)

    def take(i, c):
        row = z - 1 - i
        for kind in range(kinds):
            arrival(kind, row * inner + x).wait_recv()

            @pl.when(z < outer - 1)
            def _():
                onward(kind, row).start()

            if inner == 2:
                across(kind, row).start()
        return c

    @pl.when(z > 0)
    def _():
        take(0, 0)

    if inner == 2:
        @pl.when(x == 1)
        def _():
            for kind in range(kinds):
                arrival(kind, partner).wait_recv()
            attend(kbuf[partner], vbuf[partner], seen(sbuf[partner]), False)

    lax.fori_loop(1, z, take, 0)

    def step(i, c):
        row = z - 1 - i
        if inner == 2:
            for kind in range(kinds):
                arrival(kind, row * inner + 1 - x).wait_recv()
        first = row * inner
        kk = kbuf[pl.ds(first, inner)].reshape(inner * rows, width)
        vv = vbuf[pl.ds(first, inner)].reshape(inner * rows, width)
        vis = jnp.concatenate(
            [jnp.where(seen(sbuf[first + i]), 1, 0) for i in range(inner)], axis=1) == 1
        attend(kk, vv, vis, False)
        return c

    lax.fori_loop(0, z, step, 0)

    left = lax.broadcasted_iota(jnp.int32, (rows, width), 1) < half
    for g in range(groups):
        for i in range(per_group):
            a = acc[g, i]
            b = acc[g, per_group + i]
            total = pltpu.roll(jnp.where(left, b, a), half, 1)
            at = (g * per_group + i) * width
            o_ref[:, at:at + width] = (jnp.where(left, a, b) / total).astype(o_ref.dtype)

    if inner == 2:
        @pl.when(x == 0)
        def _():
            for kind in range(kinds):
                across(kind, z).wait_send()

        def drain_row(row, c):
            for kind in range(kinds):
                across(kind, row).wait_send()
            return c

        lax.fori_loop(0, z, drain_row, 0)

    @pl.when(z < outer - 1)
    def _():
        def drain_column(row, c):
            for kind in range(kinds):
                onward(kind, row).wait_send()
            return c

        lax.fori_loop(0, z + 1, drain_column, 0)


def per_device(n, queries, key_matrix, value_matrix, segment_ids):
    rows, width = key_matrix.shape
    inner = 2 if n % 2 == 0 else 1
    groups = width // HEAD_WIDTH
    heads = queries.shape[1] // HEAD_WIDTH // groups
    return pl.pallas_call(
        functools.partial(kernel, n, inner),
        out_shape=pltpu.VMEM(queries.shape, jnp.bfloat16),
        in_specs=[pl.BlockSpec(memory_space=pl.ANY)] * 4,
        out_specs=pl.BlockSpec(memory_space=pltpu.VMEM),
        scratch_shapes=[
            pltpu.VMEM(queries.shape, jnp.bfloat16),
            pltpu.VMEM((n, rows, width), jnp.bfloat16),
            pltpu.VMEM((n, rows, width), jnp.bfloat16),
            pltpu.VMEM((n, 1, rows), jnp.int32),
            pltpu.VMEM((groups, heads, rows, width), jnp.bfloat16),
            pltpu.VMEM((groups, heads, rows, rows), jnp.float32),
            pltpu.VMEM((groups, heads, rows, width), jnp.float32),
            pltpu.SemaphoreType.DMA((4,)),
            pltpu.SemaphoreType.DMA((1 + 2 * PIECES, n // inner)),
            pltpu.SemaphoreType.DMA((1 + 2 * PIECES, n // inner)),
            pltpu.SemaphoreType.DMA((1 + 2 * PIECES, n)),
        ],
        compiler_params=pltpu.CompilerParams(collective_id=0, has_side_effects=True),
    )(queries, key_matrix, value_matrix, segment_ids.reshape(1, rows))


def solution(mesh):
    blocks = P(("sweep", "seq"), "head")
    return jax.shard_map(
        functools.partial(per_device, mesh.shape["seq"]),
        mesh=mesh,
        in_specs=(blocks, blocks, blocks, P(("sweep", "seq"))),
        out_specs=blocks,
        check_vma=False,
    )
```

```python
import functools
import math

import jax
import jax.numpy as jnp
from jax import lax
from jax.experimental import pallas as pl
from jax.experimental.pallas import tpu as pltpu
from jax.sharding import PartitionSpec as P

HEAD_WIDTH = 64
NEG_FILL = -1e30
MESH = pl.DeviceIdType.MESH
PIECES = 2


def kernel(n, inner, q_hbm, k_hbm, v_hbm, s_hbm, o_ref, qv, kbuf, vbuf, sbuf, qm, run_max, acc,
           in_sem, col_sem, row_sem, recv_sem):
    rows = k_hbm.shape[0]
    width = k_hbm.shape[1]
    half = HEAD_WIDTH
    groups = width // half
    tiles = q_hbm.shape[1] // width
    per_group = tiles // groups
    outer = n // inner
    me = lax.axis_index("seq")
    z = me // inner
    x = me % inner
    partner = z * inner + (inner - 1 - x)
    kinds = 1 + 2 * PIECES
    size = rows // PIECES

    def piece(kind, block):
        if kind == 0:
            return sbuf.at[block]
        buf = kbuf if kind <= PIECES else vbuf
        return buf.at[block, pl.ds((kind - 1) % PIECES * size, size)]


    loads = [
        pltpu.make_async_copy(src, dst, in_sem.at[i])
        for i, (src, dst) in enumerate(
            ((s_hbm, sbuf.at[me]), (k_hbm, kbuf.at[me]), (v_hbm, vbuf.at[me]), (q_hbm, qv))
        )
    ]
    for load in loads:
        load.start()

    barrier = pltpu.get_barrier_semaphore()

    if inner == 2:
        pl.semaphore_signal(barrier, inc=1, device_id={"seq": partner}, device_id_type=MESH)

    @pl.when(z > 0)
    def _():
        pl.semaphore_signal(barrier, inc=1, device_id={"seq": me - inner}, device_id_type=MESH)

    pl.semaphore_wait(barrier, inner - 1 + jnp.where(z < outer - 1, 1, 0))

    def onward(kind, row):
        block = row * inner + x
        return pltpu.make_async_remote_copy(
            src_ref=piece(kind, block), dst_ref=piece(kind, block),
            send_sem=col_sem.at[kind, row], recv_sem=recv_sem.at[kind, block],
            device_id={"seq": me + inner}, device_id_type=MESH)

    def across(kind, row):
        block = row * inner + x
        return pltpu.make_async_remote_copy(
            src_ref=piece(kind, block), dst_ref=piece(kind, block),
            send_sem=row_sem.at[kind, row], recv_sem=recv_sem.at[kind, block],
            device_id={"seq": partner}, device_id_type=MESH)

    def arrival(kind, block):
        return pltpu.make_async_remote_copy(
            src_ref=piece(kind, block), dst_ref=piece(kind, block),
            send_sem=in_sem.at[0], recv_sem=recv_sem.at[kind, block],
            device_id={"seq": partner}, device_id_type=MESH)

    for kind in range(kinds):
        if kind in (0, 1, 1 + PIECES):
            loads[(0, 1, 1 + PIECES).index(kind)].wait()

        @pl.when(z < outer - 1)
        def _():
            onward(kind, z).start()

        if inner == 2:
            @pl.when(x == 0)
            def _():
                across(kind, z).start()

    loads[3].wait()

    scale = 1.0 / math.sqrt(half)
    zeros = jnp.zeros((rows, half), jnp.bfloat16)
    for g in range(groups):
        for i in range(per_group):
            at = (g * per_group + i) * width
            lo = (qv[:, at:at + half] * scale).astype(jnp.bfloat16)
            hi = (qv[:, at + half:at + width] * scale).astype(jnp.bfloat16)
            qm[g, i] = jnp.concatenate([lo, zeros], axis=1)
            qm[g, per_group + i] = jnp.concatenate([zeros, hi], axis=1)

    seg_q = jnp.transpose(jnp.broadcast_to(sbuf[me], (rows, rows)))

    def attend(kk, load_values, vis, first):
        vv = None
        count = kk.shape[0]
        bias = jnp.where(vis, 0.0, NEG_FILL).astype(jnp.float32)
        ones = jnp.ones((count, half), jnp.bfloat16)
        for g in range(groups):
            kg = kk[:, g * half:(g + 1) * half]
            kd = jnp.concatenate([kg, kg], axis=1)
            heads = 2 * per_group
            s = lax.dot_general(
                qm[g].reshape(heads * rows, width), kd, (((1,), (1,)), ((), ())),
                preferred_element_type=jnp.float32)
            s = s.reshape(heads, rows, count) + bias[None]
            top = jnp.max(s, axis=-1, keepdims=True)
            if first:
                new = jnp.broadcast_to(top, (heads, rows, rows))
            else:
                old = run_max[g]
                new = jnp.maximum(old, top)
            run_max[g] = new
            p = jnp.exp(s - jnp.concatenate([new] * (count // rows), axis=-1)).astype(jnp.bfloat16)
            if vv is None:
                vv = load_values()
            vg = vv[:, g * half:(g + 1) * half]
            sides = (jnp.concatenate([vg, ones], axis=1), jnp.concatenate([ones, vg], axis=1))
            for side in range(2):
                part = slice(side * per_group, (side + 1) * per_group)
                mixed = jnp.dot(
                    p[part].reshape(per_group * rows, count), sides[side],
                    preferred_element_type=jnp.float32).reshape(per_group, rows, width)
                if first:
                    acc[g, part] = mixed
                else:
                    acc[g, part] = acc[g, part] * jnp.exp(old[part] - new[part]) + mixed

    row_at = lax.broadcasted_iota(jnp.int32, (rows, rows), 0)
    col_at = lax.broadcasted_iota(jnp.int32, (rows, rows), 1)
    seg_k = jnp.broadcast_to(sbuf[me], (rows, rows))
    attend(kbuf[me], lambda: vbuf[me], (col_at <= row_at) & ((seg_k == seg_q) | (seg_k == 0)), True)

    def seen(seg):
        seg = jnp.broadcast_to(seg, (rows, rows))
        return (seg == seg_q) | (seg == 0)

    def take(i, c):
        row = z - 1 - i
        for kind in range(kinds):
            arrival(kind, row * inner + x).wait_recv()

            @pl.when(z < outer - 1)
            def _():
                onward(kind, row).start()

            if inner == 2:
                across(kind, row).start()
        return c

    @pl.when(z > 0)
    def _():
        take(0, 0)

    lax.fori_loop(1, z, take, 0)

    def values_of(block, first, count):
        def load():
            if inner == 2:
                for kind in range(1 + PIECES, kinds):
                    arrival(kind, block).wait_recv()
            return vbuf[pl.ds(first, count)].reshape(count * rows, width)

        return load

    if inner == 2:
        @pl.when(x == 1)
        def _():
            for kind in range(1 + PIECES):
                arrival(kind, partner).wait_recv()
            attend(kbuf[partner], values_of(partner, partner, 1), seen(sbuf[partner]), False)

    def step(i, c):
        row = z - 1 - i
        if inner == 2:
            for kind in range(1 + PIECES):
                arrival(kind, row * inner + 1 - x).wait_recv()
        first = row * inner
        kk = kbuf[pl.ds(first, inner)].reshape(inner * rows, width)
        vis = jnp.concatenate(
            [jnp.where(seen(sbuf[first + i]), 1, 0) for i in range(inner)], axis=1) == 1
        attend(kk, values_of(first + 1 - x, first, inner), vis, False)
        return c

    lax.fori_loop(0, z, step, 0)

    left = lax.broadcasted_iota(jnp.int32, (rows, width), 1) < half
    for g in range(groups):
        for i in range(per_group):
            a = acc[g, i]
            b = acc[g, per_group + i]
            total = pltpu.roll(jnp.where(left, b, a), half, 1)
            at = (g * per_group + i) * width
            o_ref[:, at:at + width] = (jnp.where(left, a, b) / total).astype(o_ref.dtype)

    if inner == 2:
        @pl.when(x == 0)
        def _():
            for kind in range(kinds):
                across(kind, z).wait_send()

        def drain_row(row, c):
            for kind in range(kinds):
                across(kind, row).wait_send()
            return c

        lax.fori_loop(0, z, drain_row, 0)

    @pl.when(z < outer - 1)
    def _():
        def drain_column(row, c):
            for kind in range(kinds):
                onward(kind, row).wait_send()
            return c

        lax.fori_loop(0, z + 1, drain_column, 0)


def per_device(n, queries, key_matrix, value_matrix, segment_ids):
    rows, width = key_matrix.shape
    inner = 2 if n % 2 == 0 else 1
    groups = width // HEAD_WIDTH
    heads = queries.shape[1] // HEAD_WIDTH // groups
    return pl.pallas_call(
        functools.partial(kernel, n, inner),
        out_shape=pltpu.VMEM(queries.shape, jnp.bfloat16),
        in_specs=[pl.BlockSpec(memory_space=pl.ANY)] * 4,
        out_specs=pl.BlockSpec(memory_space=pltpu.VMEM),
        scratch_shapes=[
            pltpu.VMEM(queries.shape, jnp.bfloat16),
            pltpu.VMEM((n, rows, width), jnp.bfloat16),
            pltpu.VMEM((n, rows, width), jnp.bfloat16),
            pltpu.VMEM((n, 1, rows), jnp.int32),
            pltpu.VMEM((groups, heads, rows, width), jnp.bfloat16),
            pltpu.VMEM((groups, heads, rows, rows), jnp.float32),
            pltpu.VMEM((groups, heads, rows, width), jnp.float32),
            pltpu.SemaphoreType.DMA((4,)),
            pltpu.SemaphoreType.DMA((1 + 2 * PIECES, n // inner)),
            pltpu.SemaphoreType.DMA((1 + 2 * PIECES, n // inner)),
            pltpu.SemaphoreType.DMA((1 + 2 * PIECES, n)),
        ],
        compiler_params=pltpu.CompilerParams(collective_id=0, has_side_effects=True),
    )(queries, key_matrix, value_matrix, segment_ids.reshape(1, rows))


def solution(mesh):
    blocks = P(("sweep", "seq"), "head")
    return jax.shard_map(
        functools.partial(per_device, mesh.shape["seq"]),
        mesh=mesh,
        in_specs=(blocks, blocks, blocks, P(("sweep", "seq"))),
        out_specs=blocks,
        check_vma=False,
    )
```
